32 devices in a mesh: dp: 4 (over z), table: 8 (over y, x, core).
Axes of the slice: x: 2, y: 2, z: 4, core: 2. Of those that a mesh axis runs over, the one named last changes fastest.
Arguments:
- values: bfloat16 [8192, 1024], P('table'), may hold values from -6 to 6
- first_moment: float32 [8192, 1024], P('table'), may hold values from -2 to 2
- second_moment: float32 [8192, 1024], P('table'), may hold values from 0.01 to 1
- grads: bfloat16 [256, 64, 1024], P(('dp', 'table')), may hold values from -6 to 6
- block_ids: int32 [32, 8], P(('dp', 'table')), may hold values from 0 to 127, as said below
- live_counts: int32 [32], P(('dp', 'table')), may hold values from 4 to 8
- step_count: int32 [1], replicated, may hold values from 1 to 19
Outputs:
- new_values: bfloat16 [8192, 1024], P('table')
- new_first: float32 [8192, 1024], P('table')
- new_second: float32 [8192, 1024], P('table')
The draws below stay inside these ranges and needn't reach their ends.
Inputs may be any that keep to these rules, and one draw needn't show every extreme that they name: `block_ids`: device h belongs to replica h // 8. Live ids of a device are ascending and lie in blocks of different owners (owner = id // 16), so one device sends at most one live block to any owner; in every draw some owner receives a live block from every device of a replica. The live ids of one replica name at most 2 different blocks of any one owner, and exactly 2 of some owner in every replica. Ids of dead slots are arbitrary blocks.
All inputs are finite; a program needn't handle non-finite values.
Results may differ from the reference program's by a relative error of at most 0.0004.
Values may be sent and summed in bfloat16 or wider, within the bound.
No kernel may reach another device: no remote copies, remote signals or barrier semaphores. Data moves between devices by JAX's collectives and lax.ppermute only.
A program may use at most 128 MiB of HBM per device.

```python
import math
import jax
import jax.numpy as jnp

D = 1024
BROWS = 64
SLOTS = 8
BLK_DEV = 16
NBLK = 128
ROWS = 8192
HOLDERS = 32
GSLOTS = 256


def draw_pair(key):
    key = jax.random.fold_in(key, 7)
    keys = jax.random.split(key, 7)
    owners = NBLK // BLK_DEV
    replicas = HOLDERS // owners
    holder = jnp.arange(HOLDERS, dtype=jnp.int32)
    replica = holder // owners
    column = holder % owners
    hot = jax.random.randint(keys[0], (replicas,), 0, owners)[replica]
    scores = jax.random.randint(keys[1], (HOLDERS, owners - 1), 0, 1 << 20) * owners + jnp.arange(owners - 1, dtype=jnp.int32)[None, :]
    offsets = jnp.argsort(scores, axis=1)[:, :SLOTS - 1].astype(jnp.int32) + 1
    chosen = jnp.concatenate([hot[:, None], (hot[:, None] + offsets) % owners], axis=1)
    pair_first = jax.random.randint(keys[2], (replicas, owners), 0, BLK_DEV)
    pair_second = (pair_first + 1 + jax.random.randint(keys[3], (replicas, owners), 0, BLK_DEV - 1)) % BLK_DEV
    picks = jax.random.randint(keys[4], (HOLDERS, SLOTS - 1), 0, 2)
    picks = jnp.concatenate([(column % 2)[:, None], picks], axis=1)
    option_one = pair_first[replica[:, None], chosen]
    option_two = pair_second[replica[:, None], chosen]
    local = jnp.where(picks == 0, option_one, option_two)
    named = chosen * BLK_DEV + local
    counts = jax.random.randint(keys[5], (HOLDERS,), SLOTS // 2, SLOTS + 1)
    filler = jax.random.randint(keys[6], (HOLDERS, SLOTS), 0, NBLK)
    live = jnp.arange(SLOTS, dtype=jnp.int32)[None, :] < counts[:, None]
    keyed = jnp.where(live, named, NBLK + filler)
    ordered = jnp.sort(keyed, axis=1)
    result = jnp.where(ordered < NBLK, ordered, ordered - NBLK)
    return (result.astype(jnp.int32), counts.astype(jnp.int32))


def draw_block_ids(key, part):
    return draw_pair(key)[0]


def draw_live_counts(key, part):
    return draw_pair(key)[1]


def levels(own_key, dims, shards, smallest, largest):
    level = 1.0
    for position, shards_of in shards:
        draws = jax.random.uniform(jax.random.fold_in(jax.random.fold_in(own_key, 6), position), (shards_of,), jnp.float32, smallest / len(shards), largest / len(shards))
        level = level * jnp.repeat(jnp.exp(draws), dims[position] // shards_of).reshape((-1,) + (1,) * (len(dims) - 1 - position))
    return level


def gaussian(key, extent, width, limit, shards=(), held_as=jnp.bfloat16):
    factor_of = levels(key, extent, shards, -0.22, 0.18) if shards else 1.0
    values = jax.random.normal(key, extent, jnp.float32) * width * factor_of
    return jnp.minimum(jnp.maximum(values, -limit), limit).astype(held_as)


def setup_inputs(seed: int = 0) -> dict:
    seeds = jax.random.split(jax.random.key(seed), 8)
    return {
        "values": gaussian(seeds[0], (ROWS, D), 1.0, 6.0, ((0, 8),)),
        "first_moment": gaussian(seeds[1], (ROWS, D), 0.3, 2.0, ((0, 8),), jnp.float32),
        "second_moment": jnp.clip(jnp.exp(math.log(1.0) - 4.6051702 * jax.random.uniform(seeds[2], (ROWS, D), jnp.float32) ** levels(seeds[2], (ROWS, D), ((0, 8),), -0.2, 0.2)), 0.01, 1.0),
        "grads": gaussian(seeds[3], (GSLOTS, BROWS, D), 1.0, 6.0, ((0, 32),)),
        "block_ids": draw_block_ids(jax.random.fold_in(seeds[7], 71), 0),
        "live_counts": draw_live_counts(jax.random.fold_in(seeds[7], 71), 0),
        "step_count": jax.random.randint(seeds[6], (1,), 1, 20).astype(jnp.int32),
    }


def reference(values, first_moment, second_moment, grads, block_ids, live_counts, step_count):
    live = (jnp.arange(SLOTS, dtype=jnp.int32)[None, :] < live_counts[:, None]).reshape(-1)
    flat_ids = block_ids.reshape(-1).astype(jnp.int32)
    weight = live.astype(jnp.float32)
    summed = jax.ops.segment_sum(grads.astype(jnp.float32) * weight[:, None, None], flat_ids, NBLK)
    row_grad = summed.reshape(ROWS, D)
    hits = jax.ops.segment_sum(weight, flat_ids, NBLK)
    touched = (jnp.repeat(hits, BROWS) > 0.0)[:, None]
    beta_one = 0.9
    beta_two = 0.99
    steps_done = step_count[0].astype(jnp.float32)
    first_next = beta_one * first_moment + (1.0 - beta_one) * row_grad
    second_next = beta_two * second_moment + (1.0 - beta_two) * row_grad * row_grad
    first_hat = first_next / (1.0 - jnp.power(jnp.float32(beta_one), steps_done))
    second_hat = second_next / (1.0 - jnp.power(jnp.float32(beta_two), steps_done))
    moved = values.astype(jnp.float32) - 0.05 * first_hat / (jnp.sqrt(second_hat) + 1e-08)
    new_values = jnp.where(touched, moved.astype(jnp.bfloat16), values)
    new_first = jnp.where(touched, first_next, first_moment)
    new_second = jnp.where(touched, second_next, second_moment)
    return (new_values, new_first, new_second)
```

```python
import functools
import jax
import jax.numpy as jnp
from jax import lax
from jax.experimental import pallas as pl
from jax.experimental.pallas import tpu as pltpu
from jax.sharding import PartitionSpec as P


LANES = 128
KBLK = 2
META = 16
GRAD_MAX = 6.0
TOP = 32767.0
LR = 0.05
B1 = 0.9
B2 = 0.99
EPS = 1e-08

VMEM = pl.BlockSpec(memory_space=pltpu.VMEM)
HBM = pl.BlockSpec(memory_space=pltpu.HBM)
SMEM = pl.BlockSpec(memory_space=pltpu.SMEM)


def tiles(x):
    rows, cols = x.shape[-2:]
    lead = x.shape[:-2]
    split = x.reshape(lead + (rows // 8, 8, cols // LANES, LANES))
    return split.swapaxes(-3, -2).reshape(lead + (rows * cols // LANES, LANES))


def untiles(x, cols):
    rows = x.shape[0] * LANES // cols
    split = x.reshape(rows // 8, cols // LANES, 8, LANES)
    return split.swapaxes(-3, -2).reshape(rows, cols)


def select_kernel(n, blk_here, ids_ref, count_ref, grads_ref, *refs):
    outs, (slot_of, sems) = refs[:n], refs[n:]
    slots, length = grads_ref.shape[:2]
    me = lax.axis_index("table")
    for k in range(n):
        slot_of[k] = -1
    for j in range(slots):
        @pl.when(j < count_ref[0])
        def _(j=j):
            slot_of[(ids_ref[0, j] // blk_here) ^ me] = j

    def copy(k):
        return pltpu.make_async_copy(
            grads_ref.at[jnp.maximum(slot_of[k], 0)], outs[k].at[pl.ds(0, length)], sems.at[k]
        )

    for k in range(n):
        @pl.when(slot_of[k] >= 0)
        def _(k=k):
            copy(k).start()

        slot = slot_of[k]
        local = jnp.where(slot >= 0, ids_ref[0, jnp.maximum(slot, 0)] % blk_here, -1)
        outs[k][length:, :] = jnp.full((META, LANES), local.astype(jnp.float32)).astype(jnp.bfloat16)
    for k in range(n):
        @pl.when(slot_of[k] >= 0)
        def _(k=k):
            copy(k).wait()


def stage_kernel(values_ref, first_ref, second_ref, *refs):
    outs, kept, (sems,) = refs[:3], refs[3:6], refs[6:]
    parts = 4
    pairs = []
    for i, src in enumerate((values_ref, first_ref, second_ref)):
        step = src.shape[0] // parts
        for p in range(parts):
            rows = pl.ds(p * step, step)
            read = pltpu.make_async_copy(src.at[rows], kept[i].at[rows], sems.at[0, i * parts + p])
            write = pltpu.make_async_copy(kept[i].at[rows], outs[i].at[rows], sems.at[1, i * parts + p])
            pairs.append((read, write))
    for read, _ in pairs:
        read.start()
    for read, write in pairs:
        read.wait()
        write.start()
    for _, write in pairs:
        write.wait()


def sum_kernel(cols, bound, *refs):
    ins, code_ref, acc = refs[:-2], refs[-2], refs[-1]
    length = ins[0].shape[0] - META
    group = cols * 8
    ids = [ref[length:, :].astype(jnp.float32)[:8] for ref in ins]
    big = float(1 << 20)
    low = functools.reduce(jnp.minimum, [jnp.where(i >= 0, i, big) for i in ids])
    high = functools.reduce(jnp.maximum, ids)
    second = high > low

    def add_up(r, tops):
        rows = pl.ds(pl.multiple_of(r * group, group), group)
        sums = [jnp.zeros((cols, 8, LANES), jnp.float32)] * KBLK
        for ref, i in zip(ins, ids):
            x = ref[rows, :].astype(jnp.float32).reshape(cols, 8, LANES)
            takes = (i == low, (i == high) & second)
            sums = [s + jnp.where(t[None], x, 0.0) for s, t in zip(sums, takes)]
        for j in range(KBLK):
            acc[j, rows, :] = sums[j].reshape(group, LANES)
        return tuple(jnp.maximum(t, jnp.abs(s)) for t, s in zip(tops, sums))

    zero = jnp.zeros((cols, 8, LANES), jnp.float32)
    tops = lax.fori_loop(0, length // group, add_up, (zero,) * KBLK)
    codes = [jnp.minimum(jnp.ceil(jnp.max(t, axis=1) * (TOP / bound)), TOP) for t in tops]
    inverse = [jnp.where(c > 0, (TOP * TOP / bound) / jnp.maximum(c, 1.0), 0.0) for c in codes]

    def encode(r, _):
        for j in range(KBLK):
            rows = pl.ds(pl.multiple_of(r * group, group), group)
            x = acc[j, rows, :].reshape(cols, 8, LANES) * inverse[j][:, None, :]
            to = pl.ds(pl.multiple_of(j * length + r * group, group), group)
            code_ref[to, :] = jnp.round(x).astype(jnp.int32).astype(jnp.int16).reshape(group, LANES)
        return 0

    lax.fori_loop(0, length // group, encode, 0)
    at = KBLK * length
    code_ref[at : at + KBLK * cols, :] = jnp.concatenate(codes, axis=0).astype(jnp.int32).astype(jnp.int16)
    at += KBLK * cols
    named = [jnp.where(high < 0, -1.0, low), jnp.where(second, high, -1.0)]
    code_ref[at : at + KBLK * 8, :] = jnp.concatenate(named, axis=0).astype(jnp.int32).astype(jnp.int16)


def adam_kernel(n, cols, bound, step_ref, *refs):
    coded, kept, refs = refs[:n], refs[n : n + 3], refs[n + 6 :]
    outs, (ids, todo, new_values, new_first, new_second, sems) = refs[:3], refs[3:]
    length = new_first.shape[1]
    group = cols * 8
    entries = n * KBLK
    at = KBLK * length
    found = []
    for k in range(n):
        named = coded[k][at + KBLK * cols :, :].astype(jnp.int32).astype(jnp.float32)
        for j in range(KBLK):
            found.append(jnp.max(named[j * 8 : j * 8 + 8]).astype(jnp.int32))
    for e in range(entries):
        ids[e] = found[e]
        fresh = found[e] >= 0
        for other in found[:e]:
            fresh = fresh & (found[e] != other)
        todo[e] = fresh.astype(jnp.int32)

    power_one, power_two = lax.fori_loop(
        0, step_ref[0], lambda i, p: (p[0] * jnp.float32(B1), p[1] * jnp.float32(B2)), (jnp.float32(1.0), jnp.float32(1.0))
    )
    ones = jnp.ones((8, LANES), jnp.float32)
    rate = (LR / (ones - power_one * ones))[None]
    scale_two = (1.0 / (ones - power_two * ones))[None]

    def copies(e):
        block = pl.ds(pl.multiple_of(ids[e] * length, length), length)
        return [
            pltpu.make_async_copy(src.at[e], dst.at[block], sems.at[i, e])
            for i, (src, dst) in enumerate(zip((new_values, new_first, new_second), outs))
        ]

    def entry(e, _):
        @pl.when(todo[e] > 0)
        def _():
            block = ids[e]
            offsets, steps = [], []
            for k in range(n):
                is_second = ids[k * KBLK + 1] == block
                present = is_second | (ids[k * KBLK] == block)
                offsets.append(jnp.where(is_second, length, 0))
                size = jnp.where(present, jnp.float32(bound / (TOP * TOP)), jnp.float32(0.0))
                scale = coded[k][at : at + KBLK * cols, :].astype(jnp.int32).astype(jnp.float32)
                steps.append(jnp.where(is_second, scale[cols:], scale[:cols]) * size)

            for c in range(0, cols, 2):
                here = [s[c : c + 2][:, None, :] for s in steps]

                def rows_of(r, _, c=c, here=here):
                    row = r * group + c * 8
                    terms = []
                    for k in range(n):
                        q = coded[k][pl.ds(pl.multiple_of(offsets[k] + row, 16), 16), :]
                        terms.append(q.astype(jnp.int32).astype(jnp.float32).reshape(2, 8, LANES) * here[k])
                    while len(terms) > 1:
                        terms = [terms[i] + terms[i + 1] for i in range(0, len(terms), 2)]
                    grad = terms[0]
                    source = pl.ds(pl.multiple_of(block * length + row, 16), 16)
                    target = pl.ds(pl.multiple_of(row, 16), 16)
                    value, first, square = [
                        ref[source, :].astype(jnp.float32).reshape(2, 8, LANES) for ref in kept
                    ]
                    first_next = B1 * first + (1.0 - B1) * grad
                    second_next = B2 * square + (1.0 - B2) * grad * grad
                    moved = value - rate * first_next / (jnp.sqrt(second_next * scale_two) + EPS)
                    new_values[e, target, :] = moved.reshape(16, LANES).astype(jnp.bfloat16)
                    new_first[e, target, :] = first_next.reshape(16, LANES)
                    new_second[e, target, :] = second_next.reshape(16, LANES)
                    return 0

                lax.fori_loop(0, length // group, rows_of, 0, unroll=2)
            for copy in copies(e):
                copy.start()

        return 0

    lax.fori_loop(0, entries, entry, 0)

    def finish(e, _):
        @pl.when(todo[e] > 0)
        def _():
            for copy in copies(e):
                copy.wait()

        return 0

    lax.fori_loop(0, entries, finish, 0)


def per_device(values, first_moment, second_moment, grads, block_ids, live_counts, step_count):
    owners = lax.axis_size("table")
    replicas = lax.axis_size("dp")
    slots, brows, width = grads.shape
    blk_here = values.shape[0] // brows
    cols = width // LANES
    length = brows * cols
    bound = GRAD_MAX * owners
    flat = [tiles(x) for x in (values, first_moment, second_moment)]

    outgoing = pl.pallas_call(
        functools.partial(select_kernel, owners, blk_here),
        in_specs=[SMEM, SMEM, HBM],
        out_specs=[VMEM] * owners,
        out_shape=[pltpu.VMEM((length + META, LANES), jnp.bfloat16)] * owners,
        scratch_shapes=[pltpu.SMEM((owners,), jnp.int32), pltpu.SemaphoreType.DMA((owners,))],
        compiler_params=pltpu.CompilerParams(vmem_limit_bytes=2 << 20),
        name="select",
    )(block_ids, live_counts, tiles(grads))

    def exchange(x, axis, size, k):
        return lax.ppermute(x, axis, [(i, i ^ k) for i in range(size)])

    order = sorted(range(1, owners), key=lambda k: (-bin(k >> 1).count("1"), k))
    incoming = [outgoing[0]] + [exchange(outgoing[k], "table", owners, k) for k in order]

    staged = pl.pallas_call(
        stage_kernel,
        in_specs=[HBM] * 3,
        out_specs=[HBM] * 3 + [VMEM] * 3,
        out_shape=[jax.ShapeDtypeStruct(x.shape, x.dtype) for x in flat]
        + [pltpu.VMEM(x.shape, x.dtype) for x in flat],
        scratch_shapes=[pltpu.SemaphoreType.DMA((2, 12))],
        compiler_params=pltpu.CompilerParams(vmem_limit_bytes=2 << 20),
        name="stage",
    )(*flat)

    code_rows = KBLK * (length + cols + 8)
    coded = pl.pallas_call(
        functools.partial(sum_kernel, cols, bound),
        in_specs=[VMEM] * owners,
        out_specs=VMEM,
        out_shape=pltpu.VMEM((code_rows, LANES), jnp.int16),
        scratch_shapes=[pltpu.VMEM((KBLK, length, LANES), jnp.float32)],
        compiler_params=pltpu.CompilerParams(vmem_limit_bytes=4 << 20),
        name="sum",
    )(*incoming)
    arrived = [coded] + [exchange(coded, "dp", replicas, k) for k in range(1, replicas)]

    entries = replicas * KBLK
    out = pl.pallas_call(
        functools.partial(adam_kernel, replicas, cols, bound),
        in_specs=[SMEM] + [VMEM] * (replicas + 3) + [HBM] * 3,
        out_specs=[HBM] * 3,
        out_shape=[jax.ShapeDtypeStruct(x.shape, x.dtype) for x in flat],
        scratch_shapes=[
            pltpu.SMEM((entries,), jnp.int32),
            pltpu.SMEM((entries,), jnp.int32),
            pltpu.VMEM((entries, length, LANES), jnp.bfloat16),
            pltpu.VMEM((entries, length, LANES), jnp.float32),
            pltpu.VMEM((entries, length, LANES), jnp.float32),
            pltpu.SemaphoreType.DMA((3, entries)),
        ],
        input_output_aliases={1 + replicas + 3 + i: i for i in range(3)},
        compiler_params=pltpu.CompilerParams(vmem_limit_bytes=12 << 20),
        name="adam",
    )(step_count, *arrived, *staged[3:], *staged[:3])
    return tuple(untiles(x, width) for x in out)


def solution(mesh):
    in_specs = (
        P("table", None),
        P("table", None),
        P("table", None),
        P(("dp", "table"), None, None),
        P(("dp", "table"), None),
        P(("dp", "table")),
        P(),
    )
    out_specs = (P("table", None), P("table", None), P("table", None))
    return jax.shard_map(
        per_device, mesh=mesh, in_specs=in_specs, out_specs=out_specs, check_vma=False
    )
```
